32 devices in a mesh: owner: 4 (over z), rows: 8 (over y, x, core).
Axes of the slice: x: 2, y: 2, z: 4, core: 2. Of those that a mesh axis runs over, the one named last changes fastest.
Arguments:
- w_gate: float32 [128, 2048, 768], P('owner', 'rows'), may hold values from -0.1875 to 0.1875
- w_up: float32 [128, 2048, 768], P('owner', 'rows'), may hold values from -0.1875 to 0.1875
- router_weight: float32 [2048, 128], P('rows', 'owner'), may hold values from -0.125 to 0.125
- router_gain: float32 [2048], P('rows'), may hold values from 0.25 to 1.75
Outputs:
- serve_gate: bfloat16 [128, 2048, 768], P('owner', None, 'rows')
- serve_up: bfloat16 [128, 2048, 768], P('owner', None, 'rows')
- scale_gate: float32 [128, 768], P('owner', 'rows')
- scale_up: float32 [128, 768], P('owner', 'rows')
- serve_router: bfloat16 [2048, 128], replicated
The draws below stay inside these ranges and needn't reach their ends.
All inputs are finite; a program needn't handle non-finite values. Where the reference program divides by a largest or mean magnitude, that divisor is 1e-20 or more.
Results may differ from the reference program's by a relative error of at most 0.001.
Values may be sent and summed in bfloat16 or wider, within the bound.
No kernel may reach another device: no remote copies, remote signals or barrier semaphores. Data moves between devices by JAX's collectives and lax.ppermute only.
A program may use at most 192 MiB of HBM per device.

```python
import jax
import jax.numpy as jnp

EXPERTS = 128
D_MODEL = 2048
D_EXPERT = 768


def spiked(result, key, source, target, blocks, factor):
    owner, partner = [(jnp.arange(result.shape[dim]) // (result.shape[dim] // blocks)).reshape([-1 if axis == dim else 1 for axis in range(result.ndim)]) for dim in (source, target)]
    chosen = jax.random.permutation(key, blocks)[partner]
    strong = (owner == chosen) | (owner == (partner + blocks // 2) % blocks)
    return jnp.where(strong, factor * result, result)


def shard_levels(stream_key, extent, cuts, least, high):
    factor_of = 1.0
    for axis_at, parts in cuts:
        draws = jax.random.uniform(jax.random.fold_in(jax.random.fold_in(stream_key, 6), axis_at), (parts,), jnp.float32, least / len(cuts), high / len(cuts))
        factor_of = factor_of * jnp.repeat(jnp.exp(draws), extent[axis_at] // parts).reshape((-1,) + (1,) * (len(extent) - 1 - axis_at))
    return factor_of


def bell_draw(key, extent, spread, reach, cuts=(), held_as=jnp.bfloat16):
    loudness = shard_levels(key, extent, cuts, -0.22, 0.18) if cuts else 1.0
    entries = jax.random.normal(key, extent, jnp.float32) * spread * loudness
    return jnp.minimum(jnp.maximum(entries, -reach), reach).astype(held_as)


def bell_draw_with(key, dims, deviation, most, pieces, heavy, held_as=jnp.bfloat16):
    drawn = deviation * jax.random.normal(key, dims, jnp.float32)
    if pieces:
        drawn = drawn * shard_levels(key, dims, pieces, -0.22, 0.18)
    return jnp.clip(spiked(drawn, jax.random.fold_in(key, 3), *heavy), -most, most).astype(held_as)


def setup_inputs(seed: int = 0) -> dict:
    keys = jax.random.split(jax.random.key(seed), 5)
    w_gate = bell_draw_with(keys[0], (EXPERTS, D_MODEL, D_EXPERT), D_MODEL ** -0.5, 0.1875, ((0, 4), (1, 8)), (1, 2, 8, 2.0), jnp.float32)
    w_up = bell_draw_with(keys[1], (EXPERTS, D_MODEL, D_EXPERT), D_MODEL ** -0.5, 0.1875, ((0, 4), (1, 8)), (1, 2, 8, 2.0), jnp.float32)
    router_weight = bell_draw(keys[2], (D_MODEL, EXPERTS), D_MODEL ** -0.5, 0.125, ((0, 8), (1, 4)), jnp.float32)
    router_gain = jnp.clip(1.0 + 0.15 * jax.random.normal(keys[3], (D_MODEL,), jnp.float32), 0.25, 1.75)
    return {"w_gate": w_gate, "w_up": w_up, "router_weight": router_weight, "router_gain": router_gain}


def reference(w_gate, w_up, router_weight, router_gain):
    scale_gate = jnp.sum(jnp.abs(w_gate), axis=1) / D_MODEL
    serve_gate = (w_gate / jnp.expand_dims(scale_gate, 1)).astype(jnp.bfloat16)
    scale_up = jnp.sum(jnp.abs(w_up), axis=1) / D_MODEL
    serve_up = (w_up / jnp.expand_dims(scale_up, 1)).astype(jnp.bfloat16)
    serve_router = (router_weight * router_gain[:, None]).astype(jnp.bfloat16)
    return serve_gate, serve_up, scale_gate, scale_up, serve_router
```

```python
import functools

import jax
import jax.numpy as jnp
from jax import lax
from jax.experimental import pallas as pl
from jax.experimental.pallas import tpu as pltpu
from jax.sharding import PartitionSpec as P


CHUNKS = (2, 4, 6, 6, 6, 4, 2, 1, 1)
ROUTER_CHUNK = 1
SPAN, BASE = 251.0, 125.0
SIDE = 8
LANES = 128


def pack_kernel(parts, count, routed, me, wg, wu, *rest):
    rw, gain, rest = (rest[0], rest[1], rest[2:]) if routed else (None, None, rest)
    outs, after, turned, tops = rest[:parts], rest[parts], rest[parts + 1], rest[parts + 2]
    after[0] = me[0]
    height = turned.shape[0] // parts
    e = pl.program_id(0)
    starts = [pl.multiple_of((me[0] ^ k) * height, height) for k in range(parts)]

    @pl.when(e < count)
    def _():
        for t, w in enumerate((wg, wu)):
            x = w[0]
            mag = jnp.abs(x)
            top = jnp.max(mag, axis=0, keepdims=True)
            top = (top * 1.0079).astype(jnp.bfloat16).astype(jnp.float32)
            tops[t, pl.ds(e, 1), :] = top
            part = mag * jnp.where(top > 1e-30, 1.0 / top, 0.0)
            root = part * lax.rsqrt(jnp.maximum(part, 1e-30))
            code = jnp.exp2(root * SPAN - BASE)
            code = jnp.where(x < 0, -code, code)
            turned[...] = code.T.astype(jnp.bfloat16)
            for k in range(parts):
                outs[k][t * height : (t + 1) * height, :] = turned[pl.ds(starts[k], height), :]

    @pl.when(e == count)
    def _():
        cols = turned.shape[0]
        at = 0
        if routed:
            at = rw.shape[0]
            made = (rw[...] * gain[...]).astype(jnp.bfloat16)
        for k in range(parts):
            if routed:
                outs[k][:at, :] = made
            for t in range(2):
                row = pltpu.roll(tops[t], cols - starts[k], 1)[:, :LANES]
                outs[k][at : at + SIDE, t * LANES : (t + 1) * LANES] = row.astype(jnp.bfloat16)


def pack(w_gate, w_up, routing, me, first, count, parts):
    _, rows, cols = w_gate.shape
    height = cols // parts
    last = count - 1
    block = pl.BlockSpec((1, rows, cols), lambda e, me: (first + jnp.minimum(e, last), 0, 0))
    whole = [pl.BlockSpec(r.shape, lambda e, me: (0, 0)) for r in routing]
    piece = pl.BlockSpec((2 * height, rows), lambda e, me: (e, 0))
    length = 2 * height * count + SIDE + (routing[0].shape[0] if routing else 0)
    return pl.pallas_call(
        functools.partial(pack_kernel, parts, count, bool(routing)),
        grid_spec=pltpu.PrefetchScalarGridSpec(
            num_scalar_prefetch=1,
            grid=(count + 1,),
            in_specs=[block, block] + whole,
            out_specs=[piece] * parts + [pl.BlockSpec(memory_space=pltpu.SMEM)],
            scratch_shapes=[
                pltpu.VMEM((cols, rows), jnp.bfloat16),
                pltpu.VMEM((2, SIDE, cols), jnp.float32),
            ],
        ),
        out_shape=[jax.ShapeDtypeStruct((length, rows), jnp.bfloat16)] * parts
        + [jax.ShapeDtypeStruct((1,), jnp.int32)],
        name="pack",
    )(me, w_gate, w_up, *routing)


def unpack_kernel(parts, first, routed, held, d_model, me, *refs):
    bulk, side, refs = refs[:parts], refs[parts : 2 * parts], refs[2 * parts :]
    if routed:
        routes, refs = refs[:parts], refs[parts:]
    if held:
        scales_in, refs = refs[2:4], refs[4:]
    outs, scales, refs = refs[:2], refs[2:4], refs[4:]
    tops = refs[-1]
    e = pl.program_id(0)
    height, rows = bulk[0].shape[0] // 2, bulk[0].shape[1]
    starts = [pl.multiple_of((me[0] ^ k) * rows, rows) for k in range(parts)]

    @pl.when(e == 0)
    def _():
        for t in range(2):
            if held:
                scales[t][...] = scales_in[t][...]
            for k in range(parts):
                tops[t, k * SIDE : (k + 1) * SIDE, :] = side[k][
                    :, t * LANES : (t + 1) * LANES
                ].astype(jnp.float32)
        if routed:
            for k in range(parts):
                refs[0][:, pl.ds(starts[k], rows)] = routes[k][...]

    step = 16
    down = lax.broadcasted_iota(jnp.int32, (step, LANES), 0)
    across = lax.broadcasted_iota(jnp.int32, (step, LANES), 1)
    for t in range(2):
        top = jnp.concatenate([tops[t, pl.ds(k * SIDE + e, 1), :] for k in range(parts)], axis=0)
        top = (top * (1.0 / (SPAN * SPAN))).T
        scale = jnp.zeros((1, LANES), jnp.float32)
        for r in range(0, height, step):
            values, total = [], jnp.zeros((step, rows), jnp.float32)
            for k in range(parts):
                code = bulk[k][t * height + r : t * height + r + step, :].astype(jnp.float32)
                root = jnp.log2(jnp.abs(code)) + BASE
                mag = root * root * top[r : r + step, k : k + 1]
                total = total + mag
                values.append(jnp.where(code < 0, -mag, mag))
            mean = jnp.sum(total, axis=1, keepdims=True) / d_model
            inverse = 1.0 / mean
            for k in range(parts):
                outs[t][0, r : r + step, pl.ds(starts[k], rows)] = (values[k] * inverse).astype(
                    jnp.bfloat16
                )
            scale = scale + jnp.sum(
                jnp.where(down + r == across, mean, 0.0), axis=0, keepdims=True
            )
        scales[t][pl.ds(first + e, 1), :] = scale[:, :height]


def unpack(pieces, held, me, first, count, experts, d_model, routes):
    parts = len(pieces)
    rows = pieces[0].shape[1]
    above = 2 * count * (pieces[0].shape[0] - SIDE - routes) // (2 * count)
    height = above // (2 * count)
    bulk = pl.BlockSpec((2 * height, rows), lambda e, me: (e, 0))
    side = pl.BlockSpec((SIDE, rows), lambda e, me: ((above + routes) // SIDE, 0))
    specs, operands = [bulk] * parts + [side] * parts, list(pieces) * 2
    if routes:
        specs += [pl.BlockSpec((routes, rows), lambda e, me: (above // routes, 0))] * parts
        operands += list(pieces)
    whole = pl.BlockSpec((experts, height), lambda e, me: (0, 0))
    aliases = {}
    if held is not None:
        aliases = {1 + len(operands) + i: i for i in range(4)}
        specs += [pl.BlockSpec(memory_space=pl.ANY)] * 2 + [whole] * 2
        operands += list(held)
    out = pl.BlockSpec((1, height, parts * rows), lambda e, me: (first + e, 0, 0))
    served = jax.ShapeDtypeStruct((experts, height, parts * rows), jnp.bfloat16)
    scale = jax.ShapeDtypeStruct((experts, height), jnp.float32)
    out_specs, out_shape = [out, out, whole, whole], [served, served, scale, scale]
    if routes:
        out_specs.append(pl.BlockSpec((routes, parts * rows), lambda e, me: (0, 0)))
        out_shape.append(jax.ShapeDtypeStruct((routes, parts * rows), jnp.bfloat16))
    return pl.pallas_call(
        functools.partial(unpack_kernel, parts, first, bool(routes), held is not None, d_model),
        grid_spec=pltpu.PrefetchScalarGridSpec(
            num_scalar_prefetch=1,
            grid=(count,),
            in_specs=specs,
            out_specs=out_specs,
            scratch_shapes=[pltpu.VMEM((2, parts * SIDE, LANES), jnp.float32)],
        ),
        out_shape=out_shape,
        input_output_aliases=aliases,
        name="unpack",
    )(me, *operands)


def exchanged(parts, d_model, w_gate, w_up, router_weight, router_gain):
    experts, rows, _ = w_gate.shape
    me = lax.axis_index("rows").astype(jnp.int32).reshape(1)
    arrived, first, turn = [], 0, me
    for c, count in enumerate(CHUNKS):
        routing = (router_weight.T, router_gain.reshape(1, rows)) if c == ROUTER_CHUNK else ()
        *pieces, turn = pack(w_gate, w_up, routing, turn, first, count, parts)
        moved = [pieces[0]]
        for k in range(1, parts):
            pairs = [(r, r ^ k) for r in range(parts)]
            moved.append(lax.ppermute(pieces[k], "rows", pairs))
        arrived.append((moved, first, count))
        first += count
    held = None
    for c, (moved, at, count) in enumerate(arrived):
        routes = router_weight.shape[1] if c == ROUTER_CHUNK else 0
        held = unpack(moved, held, me, at, count, experts, d_model, routes)
        if routes:
            *held, part = held
            whole = lax.all_gather(part, "owner", axis=0, tiled=True).T
            *held, serve_router = lax.optimization_barrier((*held, whole))
    gate, up, scale_gate, scale_up = held
    return jnp.swapaxes(gate, 1, 2), jnp.swapaxes(up, 1, 2), scale_gate, scale_up, serve_router


def plain(parts, d_model, w_gate, w_up, router_weight, router_gain):
    totals = lax.psum(tuple(jnp.sum(jnp.abs(w), axis=1) for w in (w_gate, w_up)), "rows")
    served, scales = [], []
    for w, total in zip((w_gate, w_up), totals):
        scale = total / d_model
        narrow = (w / jnp.expand_dims(scale, 1)).astype(jnp.bfloat16)
        served.append(lax.all_to_all(narrow, "rows", split_axis=2, concat_axis=1, tiled=True))
        width = scale.shape[1] // parts
        at = lax.axis_index("rows") * width
        scales.append(lax.dynamic_slice_in_dim(scale, at, width, axis=1))
    part = (router_weight * router_gain[:, None]).astype(jnp.bfloat16)
    part = lax.all_gather(part, "rows", axis=0, tiled=True)
    return (*served, *scales, lax.all_gather(part, "owner", axis=1, tiled=True))


def solution(mesh):
    parts = mesh.shape["rows"]

    def on_device(w_gate, w_up, router_weight, router_gain):
        experts, rows, cols = w_gate.shape
        fits = (
            parts & (parts - 1) == 0
            and rows == 2 * LANES
            and cols % (16 * parts) == 0
            and cols // parts <= LANES
            and router_weight.shape[1] % 16 == 0
            and (2 * cols // parts) % router_weight.shape[1] == 0
            and experts == sum(CHUNKS)
        )
        body = exchanged if fits else plain
        return body(parts, rows * parts, w_gate, w_up, router_weight, router_gain)

    return jax.shard_map(
        on_device,
        mesh=mesh,
        in_specs=(
            P("owner", "rows", None),
            P("owner", "rows", None),
            P("rows", "owner"),
            P("rows"),
        ),
        out_specs=(
            P("owner", None, "rows"),
            P("owner", None, "rows"),
            P("owner", "rows"),
            P("owner", "rows"),
            P(),
        ),
        check_vma=False,
    )
```

```python
import functools

import jax
import jax.numpy as jnp
from jax import lax
from jax.experimental import pallas as pl
from jax.experimental.pallas import tpu as pltpu
from jax.sharding import PartitionSpec as P


CHUNKS = (2, 6, 8, 8, 5, 2, 1)
ROUTER_CHUNK = 1
SPAN, BASE = 251.0, 125.0
SIDE = 8
LN2 = 0.6931471805599453
LANES = 128


def pack_kernel(parts, count, routed, me, wg, wu, *rest):
    rw, gain, rest = (rest[0], rest[1], rest[2:]) if routed else (None, None, rest)
    outs, (after, turned, tops, sides) = rest[:parts], rest[parts:]
    after[0] = me[0]
    height = turned.shape[0] // parts
    e = pl.program_id(0)
    starts = [pl.multiple_of((me[0] ^ k) * height, height) for k in range(parts)]

    @pl.when(e < count)
    def _():
        for t, w in enumerate((wg, wu)):
            x = w[0]
            mag = jnp.abs(x)
            top = jnp.max(mag, axis=0, keepdims=True)
            top = (top * 1.0079).astype(jnp.bfloat16).astype(jnp.float32)
            tops[t, pl.ds(e, 1), :] = top
            weight = jnp.where(top > 1e-30, SPAN * lax.rsqrt(jnp.maximum(top, 1e-30)), 0.0)
            root = mag * lax.rsqrt(jnp.maximum(mag, 1e-37))
            code = jnp.exp2(root * weight - BASE)
            code = jnp.where(x < 0, -code, code)
            turned[...] = code.astype(jnp.bfloat16).T
            for k in range(parts):
                outs[k][t * height : (t + 1) * height, :] = turned[pl.ds(starts[k], height), :]

    @pl.when(e == count)
    def _():
        at = 0
        if routed:
            at = rw.shape[0]
            made = (rw[...] * gain[...]).astype(jnp.bfloat16)
        for d in range(parts):
            for t in range(2):
                row = tops[t, :, d * height : (d + 1) * height]
                sides[d, :, t * LANES : t * LANES + height] = row.astype(jnp.bfloat16)
        for k in range(parts):
            if routed:
                outs[k][:at, :] = made
            outs[k][at : at + SIDE, :] = sides[me[0] ^ k]


def pack(w_gate, w_up, routing, me, first, count, parts):
    _, rows, cols = w_gate.shape
    height = cols // parts
    last = count - 1
    block = pl.BlockSpec((1, rows, cols), lambda e, me: (first + jnp.minimum(e, last), 0, 0))
    whole = [pl.BlockSpec(r.shape, lambda e, me: (0, 0)) for r in routing]
    piece = pl.BlockSpec((2 * height, rows), lambda e, me: (e, 0))
    length = 2 * height * count + SIDE + (routing[0].shape[0] if routing else 0)
    return pl.pallas_call(
        functools.partial(pack_kernel, parts, count, bool(routing)),
        grid_spec=pltpu.PrefetchScalarGridSpec(
            num_scalar_prefetch=1,
            grid=(count + 1,),
            in_specs=[block, block] + whole,
            out_specs=[piece] * parts + [pl.BlockSpec(memory_space=pltpu.SMEM)],
            scratch_shapes=[
                pltpu.VMEM((cols, rows), jnp.bfloat16),
                pltpu.VMEM((2, SIDE, cols), jnp.float32),
                pltpu.VMEM((parts, SIDE, 2 * LANES), jnp.bfloat16),
            ],
        ),
        out_shape=[jax.ShapeDtypeStruct((length, rows), jnp.bfloat16)] * parts
        + [jax.ShapeDtypeStruct((1,), jnp.int32)],
        name="pack",
    )(me, w_gate, w_up, *routing)


def unpack_kernel(parts, first, routed, held, d_model, me, *refs):
    bulk, side, refs = refs[:parts], refs[parts : 2 * parts], refs[2 * parts :]
    if routed:
        routes, refs = refs[:parts], refs[parts:]
    if held:
        scales_in, refs = refs[2:4], refs[4:]
    outs, scales, refs = refs[:2], refs[2:4], refs[4:]
    tops = refs[-1]
    e = pl.program_id(0)
    height, rows = bulk[0].shape[0] // 2, bulk[0].shape[1]
    starts = [pl.multiple_of((me[0] ^ k) * rows, rows) for k in range(parts)]

    @pl.when(e == 0)
    def _():
        for t in range(2):
            if held:
                scales[t][...] = scales_in[t][...]
            for k in range(parts):
                tops[t, k * SIDE : (k + 1) * SIDE, :] = side[k][
                    :, t * LANES : (t + 1) * LANES
                ].astype(jnp.float32)
        if routed:
            for k in range(parts):
                refs[0][:, pl.ds(starts[k], rows)] = routes[k][...]

    step = height
    down = lax.broadcasted_iota(jnp.int32, (step, LANES), 0)
    across = lax.broadcasted_iota(jnp.int32, (step, LANES), 1)
    for t in range(2):
        top = jnp.concatenate([tops[t, pl.ds(k * SIDE + e, 1), :] for k in range(parts)], axis=0)
        top = (top * (1.0 / (SPAN * LN2) ** 2)).T
        scale = jnp.zeros((1, LANES), jnp.float32)
        for r in range(0, height, step):
            values, total = [], jnp.zeros((step, rows), jnp.float32)
            for k in range(parts):
                code = bulk[k][t * height + r : t * height + r + step, :].astype(jnp.float32)
                root = jnp.log(jnp.abs(code)) + BASE * LN2
                mag = root * root * top[r : r + step, k : k + 1]
                total = total + mag
                values.append(jnp.where(code < 0, -mag, mag))
            mean = jnp.sum(total, axis=1, keepdims=True) / d_model
            inverse = 1.0 / mean
            for k in range(parts):
                outs[t][0, r : r + step, pl.ds(starts[k], rows)] = (values[k] * inverse).astype(
                    jnp.bfloat16
                )
            scale = scale + jnp.sum(
                jnp.where(down + r == across, mean, 0.0), axis=0, keepdims=True
            )
        scales[t][pl.ds(first + e, 1), :] = scale[:, :height]


def unpack(pieces, held, me, first, count, experts, d_model, routes):
    parts = len(pieces)
    rows = pieces[0].shape[1]
    above = 2 * count * (pieces[0].shape[0] - SIDE - routes) // (2 * count)
    height = above // (2 * count)
    bulk = pl.BlockSpec((2 * height, rows), lambda e, me: (e, 0))
    side = pl.BlockSpec((SIDE, rows), lambda e, me: ((above + routes) // SIDE, 0))
    specs, operands = [bulk] * parts + [side] * parts, list(pieces) * 2
    if routes:
        specs += [pl.BlockSpec((routes, rows), lambda e, me: (above // routes, 0))] * parts
        operands += list(pieces)
    whole = pl.BlockSpec((experts, height), lambda e, me: (0, 0))
    aliases = {}
    if held is not None:
        aliases = {1 + len(operands) + i: i for i in range(4)}
        specs += [pl.BlockSpec(memory_space=pl.ANY)] * 2 + [whole] * 2
        operands += list(held)
    out = pl.BlockSpec((1, height, parts * rows), lambda e, me: (first + e, 0, 0))
    served = jax.ShapeDtypeStruct((experts, height, parts * rows), jnp.bfloat16)
    scale = jax.ShapeDtypeStruct((experts, height), jnp.float32)
    out_specs, out_shape = [out, out, whole, whole], [served, served, scale, scale]
    if routes:
        out_specs.append(pl.BlockSpec((routes, parts * rows), lambda e, me: (0, 0)))
        out_shape.append(jax.ShapeDtypeStruct((routes, parts * rows), jnp.bfloat16))
    return pl.pallas_call(
        functools.partial(unpack_kernel, parts, first, bool(routes), held is not None, d_model),
        grid_spec=pltpu.PrefetchScalarGridSpec(
            num_scalar_prefetch=1,
            grid=(count,),
            in_specs=specs,
            out_specs=out_specs,
            scratch_shapes=[pltpu.VMEM((2, parts * SIDE, LANES), jnp.float32)],
        ),
        out_shape=out_shape,
        input_output_aliases=aliases,
        name="unpack",
    )(me, *operands)


def exchanged(parts, d_model, w_gate, w_up, router_weight, router_gain):
    experts, rows, _ = w_gate.shape
    me = lax.axis_index("rows").astype(jnp.int32).reshape(1)
    arrived, first, turn = [], 0, me
    for c, count in enumerate(CHUNKS):
        routing = (router_weight.T, router_gain.reshape(1, rows)) if c == ROUTER_CHUNK else ()
        *pieces, turn = pack(w_gate, w_up, routing, turn, first, count, parts)
        moved = [pieces[0]]
        for k in range(1, parts):
            pairs = [(r, r ^ k) for r in range(parts)]
            moved.append(lax.ppermute(pieces[k], "rows", pairs))
        arrived.append((moved, first, count))
        first += count
    held = None
    for c, (moved, at, count) in enumerate(arrived):
        routes = router_weight.shape[1] if c == ROUTER_CHUNK else 0
        held = unpack(moved, held, me, at, count, experts, d_model, routes)
        if routes:
            *held, part = held
            whole = lax.all_gather(part, "owner", axis=0, tiled=True).T
            *held, serve_router = lax.optimization_barrier((*held, whole))
    gate, up, scale_gate, scale_up = held
    return jnp.swapaxes(gate, 1, 2), jnp.swapaxes(up, 1, 2), scale_gate, scale_up, serve_router


def plain(parts, d_model, w_gate, w_up, router_weight, router_gain):
    totals = lax.psum(tuple(jnp.sum(jnp.abs(w), axis=1) for w in (w_gate, w_up)), "rows")
    served, scales = [], []
    for w, total in zip((w_gate, w_up), totals):
        scale = total / d_model
        narrow = (w / jnp.expand_dims(scale, 1)).astype(jnp.bfloat16)
        served.append(lax.all_to_all(narrow, "rows", split_axis=2, concat_axis=1, tiled=True))
        width = scale.shape[1] // parts
        at = lax.axis_index("rows") * width
        scales.append(lax.dynamic_slice_in_dim(scale, at, width, axis=1))
    part = (router_weight * router_gain[:, None]).astype(jnp.bfloat16)
    part = lax.all_gather(part, "rows", axis=0, tiled=True)
    return (*served, *scales, lax.all_gather(part, "owner", axis=1, tiled=True))


def solution(mesh):
    parts = mesh.shape["rows"]

    def on_device(w_gate, w_up, router_weight, router_gain):
        experts, rows, cols = w_gate.shape
        fits = (
            parts & (parts - 1) == 0
            and rows == 2 * LANES
            and cols % (16 * parts) == 0
            and cols // parts <= LANES
            and router_weight.shape[1] % 16 == 0
            and (2 * cols // parts) % router_weight.shape[1] == 0
            and experts == sum(CHUNKS)
        )
        body = exchanged if fits else plain
        return body(parts, rows * parts, w_gate, w_up, router_weight, router_gain)

    return jax.shard_map(
        on_device,
        mesh=mesh,
        in_specs=(
            P("owner", "rows", None),
            P("owner", "rows", None),
            P("rows", "owner"),
            P("rows"),
        ),
        out_specs=(
            P("owner", None, "rows"),
            P("owner", None, "rows"),
            P("owner", "rows"),
            P("owner", "rows"),
            P(),
        ),
        check_vma=False,
    )
```
